32 devices in a mesh: stn: 8 (over z, core), chan: 4 (over y, x).
Axes of the slice: x: 2, y: 2, z: 4, core: 2. Of those that a mesh axis runs over, the one named last changes fastest.
Arguments:
- voltages: bfloat16 [8, 2, 256, 131072], P('stn', None, None, 'chan'), may hold values from -6 to 6
- positions: float32 [8, 3, 256], P('stn'), may hold values from -4 to 4
- directions: float32 [3, 64], replicated, may hold values from -0.5 to 0.5
- flag_mask: int32 [8, 2, 2048], P('stn', None, 'chan'), may hold values from 0 to 1, as said below
- tapers: float32 [8, 8], P('stn'), may hold values from 0.3 to 3
- weight_index: int32 [8, 64], P('stn'), may hold values from 0 to 7
Outputs:
- beam_power: float32 [64, 131072], P('stn', 'chan')
- beam_total: float32 [64], P('stn')
The draws below stay inside these ranges and needn't reach their ends.
Inputs may be any that keep to these rules, and one draw needn't show every extreme that they name: `flag_mask`: the first block of station 0 is kept in every channel.
All inputs are finite; a program needn't handle non-finite values.
Results may differ from the reference program's by a relative error of at most 0.003.
Values sent between devices are 32-bit elements; how exact they have to be, the bound alone decides.
A program may use at most 256 MiB of HBM per device.

```python
import math
import jax
import jax.numpy as jnp
from jax import lax

DIPOLES = 256
BLOCK = 128
DBLOCKS = 2
BEAMS = 64
CHANNELS = 2048
SAMPLES = 64
STATIONS = 8
TAPERS = 8


def draw_flag_mask(key, part):
    levels = jax.random.randint(key, (STATIONS, DBLOCKS, CHANNELS), 0, 4)
    kept = (levels > 0).astype(jnp.int32)
    station_ids = lax_free_iota_station()
    return jnp.where(station_ids, jnp.int32(1), kept)


def lax_free_iota_station():
    station_ids = jnp.arange(STATIONS).astype(jnp.int32)[:, None, None]
    block_ids = jnp.arange(DBLOCKS).astype(jnp.int32)[None, :, None]
    first = (station_ids == 0) & (block_ids == 0)
    return jnp.broadcast_to(first, (STATIONS, DBLOCKS, CHANNELS))


def place_ends(values, stream_key, least, high):
    shape = values.shape
    index_at = [jax.random.randint(jax.random.fold_in(stream_key, axis), (), 0, shape[axis]) for axis in range(len(shape))]
    values = values.at[tuple(index_at)].set(least)
    longest = shape.index(max(shape))
    index_at[longest] = (index_at[longest] + 1) % shape[longest]
    return values.at[tuple(index_at)].set(high)


def shard_levels(own_key, extent, pieces, low, high):
    factor_of = 1.0
    for position, shards_of in pieces:
        heights = jax.random.uniform(jax.random.fold_in(jax.random.fold_in(own_key, 6), position), (shards_of,), jnp.float32, low / len(pieces), high / len(pieces))
        factor_of = factor_of * jnp.repeat(jnp.exp(heights), extent[position] // shards_of).reshape((-1,) + (1,) * (len(extent) - 1 - position))
    return factor_of


def scatter_about(rng, shape, scale, most, shards=(), kind=jnp.bfloat16):
    level = shard_levels(rng, shape, shards, -0.22, 0.18) if shards else 1.0
    drawn = jax.random.normal(rng, shape, jnp.float32) * scale * level
    return jnp.minimum(jnp.maximum(drawn, -most), most).astype(kind)


def setup_inputs(seed: int = 0) -> dict:
    arg_keys = jax.random.split(jax.random.key(seed), 7)
    voltages = scatter_about(arg_keys[0], (STATIONS, 2, DIPOLES, CHANNELS * SAMPLES), 1.0, 6.0, ((0, 8), (3, 4)))
    positions = jnp.clip(jax.random.uniform(arg_keys[1], (STATIONS, 3, DIPOLES), jnp.float32, -4.0, 4.0) * shard_levels(arg_keys[1], (STATIONS, 3, DIPOLES), ((0, 8),), -0.4, 0.0), -4.0, 4.0)
    directions = jnp.clip(jax.random.uniform(arg_keys[2], (3, BEAMS), jnp.float32, -0.5, 0.5), -0.5, 0.5)
    flag_mask = draw_flag_mask(jax.random.fold_in(arg_keys[6], 71), 0)
    tapers = jnp.clip(jnp.exp(math.log(3.0) - 2.3025851 * jax.random.uniform(arg_keys[4], (STATIONS, TAPERS), jnp.float32) ** shard_levels(arg_keys[4], (STATIONS, TAPERS), ((0, 8),), -0.2, 0.2)), 0.3, 3.0)
    weight_index = place_ends(jax.random.randint(arg_keys[5], (STATIONS, BEAMS), 0, TAPERS), jax.random.fold_in(arg_keys[5], 1), 0, TAPERS - 1).astype(jnp.int32)
    return dict(voltages=voltages, positions=positions, directions=directions, flag_mask=flag_mask, tapers=tapers, weight_index=weight_index)


def station_beam(volts, place, keep_flags, weight_row, directions, ratio):
    delay = directions[0][:, None] * place[0][None, :] + directions[1][:, None] * place[1][None, :] + directions[2][:, None] * place[2][None, :]
    phase = (2.0 * math.pi) * delay[:, :, None] * ratio[None, None, :]
    blocks = keep_flags.shape[0]
    keep = jnp.broadcast_to(keep_flags.astype(jnp.float32)[:, None, :], (blocks, BLOCK, keep_flags.shape[1])).reshape(blocks * BLOCK, keep_flags.shape[1])
    amplitude = weight_row[:, None, None] * keep[None, :, :]
    steer_real = (amplitude * jnp.cos(phase)).astype(jnp.bfloat16).astype(jnp.float32)
    steer_imag = (-amplitude * jnp.sin(phase)).astype(jnp.bfloat16).astype(jnp.float32)
    signal = volts.astype(jnp.float32).reshape(2, volts.shape[1], keep_flags.shape[1], -1)
    high = lax.Precision.HIGHEST
    real_part = jnp.einsum('bdc,dct->bct', steer_real, signal[0], precision=high) - jnp.einsum('bdc,dct->bct', steer_imag, signal[1], precision=high)
    imag_part = jnp.einsum('bdc,dct->bct', steer_real, signal[1], precision=high) + jnp.einsum('bdc,dct->bct', steer_imag, signal[0], precision=high)
    return jnp.stack((real_part, imag_part), axis=0)


def reference(voltages, positions, directions, flag_mask, tapers, weight_index):
    ratio = 1.0 + 0.5 * jnp.arange(CHANNELS).astype(jnp.float32) / CHANNELS
    choose = (weight_index[:, :, None] == jnp.arange(TAPERS).astype(jnp.int32)[None, None, :]).astype(jnp.float32)
    station_weight = jnp.sum(choose * tapers[:, None, :], axis=2)
    alive = jnp.sum(flag_mask, axis=1).astype(jnp.float32) * BLOCK
    counts = jnp.dot(station_weight.T, alive, precision=lax.Precision.HIGHEST)

    def add_station(total, items):
        volts, place, keep_flags, weight_row = items
        return total + station_beam(volts, place, keep_flags, weight_row, directions, ratio), None

    start = jnp.zeros((2, BEAMS, CHANNELS, SAMPLES), jnp.float32)
    partial_value, unused = lax.scan(add_station, start, (voltages, positions, flag_mask, station_weight))
    scaled = partial_value / counts[None, :, :, None]
    power = scaled[0] * scaled[0] + scaled[1] * scaled[1]
    beam_power = power.reshape(BEAMS, CHANNELS * SAMPLES)
    beam_total = jnp.sum(beam_power, axis=1)
    return beam_power, beam_total
```

```python
import functools
import math

import jax
import jax.numpy as jnp
from jax import lax
from jax.experimental import pallas as pl
from jax.experimental.pallas import tpu as pltpu
from jax.sharding import PartitionSpec as P

BLOCK = 128
LANES = 128
STEP = 8
MESH = pl.DeviceIdType.MESH


def turn(u):
    quarter = jnp.floor(u * 4.0 + 0.5)
    x = (u - quarter * 0.25) * (2.0 * math.pi)
    x2 = x * x
    s = x * (1.0 + x2 * (-1.0 / 6 + x2 * (1.0 / 120 + x2 * (-1.0 / 5040 + x2 * (1.0 / 362880)))))
    c = 1.0 + x2 * (-0.5 + x2 * (1.0 / 24 + x2 * (-1.0 / 720 + x2 * (1.0 / 40320))))
    q = quarter - 4.0 * jnp.floor(quarter * 0.25)
    odd = (q == 1.0) | (q == 3.0)
    cos = jnp.where(odd, s, c)
    sin = jnp.where(odd, c, s)
    cos = jnp.where((q == 1.0) | (q == 2.0), -cos, cos)
    sin = jnp.where(q >= 2.0, -sin, sin)
    return cos, sin


def kernel(
    dims, gap, volts, flags, delay, weight, counts_part, power, total,
    vbuf, part, peer, hop, base, fine, counts_in, counts_all, sums,
    v_sem, x_send, x_recv, h_send, h_recv, c_send, c_recv, t_send, t_recv,
):
    n, nchan, chips, rows, chan_local, samples, group, chunks, half = dims
    me = lax.axis_index("stn")
    col = lax.axis_index("chan")
    chip, core = lax.div(me, 2), lax.rem(me, 2)
    lanes = 2 * half

    def fetch(i):
        return pltpu.make_async_copy(
            volts.at[:, :, pl.ds(pl.multiple_of(i * lanes, lanes), lanes)],
            vbuf.at[lax.rem(i, 3)],
            v_sem.at[lax.rem(i, 3)],
        )

    for i in range(min(2, chunks)):
        fetch(i).start()

    barrier = pltpu.get_barrier_semaphore()
    for r in range(1, n):
        pl.semaphore_signal(barrier, 1, device_id=(lax.rem(me + r, n), col), device_id_type=MESH)
    for r in range(1, nchan):
        pl.semaphore_signal(barrier, 1, device_id=(me, lax.rem(col + r, nchan)), device_id_type=MESH)

    chan_whole = chan_local * nchan
    for i in range(STEP):
        c, s = turn(delay[...] * (0.5 * i / chan_whole))
        fine[i, 0] = c
        fine[i, 1] = -s
    sums[pl.ds(col, 1)] = jnp.zeros((1, rows, LANES), jnp.float32)

    pl.semaphore_wait(barrier, n - 1 + nchan - 1)

    def counts_copy(r):
        to = lax.rem(me + r, n)
        return pltpu.make_async_remote_copy(
            src_ref=counts_part.at[to], dst_ref=counts_in.at[r - 1],
            send_sem=c_send.at[r - 1], recv_sem=c_recv.at[r - 1],
            device_id=(to, col), device_id_type=MESH,
        )

    for r in range(1, n):
        counts_copy(r).start()

    def peer_copy(i):
        return pltpu.make_async_remote_copy(
            src_ref=part.at[i, 1 - core], dst_ref=peer.at[i],
            send_sem=x_send.at[i], recv_sem=x_recv.at[i],
            device_id=(chip * 2 + 1 - core, col), device_id_type=MESH,
        )

    def hop_copy(i, way, k):
        to = lax.rem(chip + (1 if way == 0 else chips - 1), chips) * 2 + core
        if k == 0:
            block = lax.rem(chip + (chips - 1 if way == 0 else 1), chips)
            src = peer.at[i, way, block]
        else:
            src = hop.at[way, k - 1, i]
        return pltpu.make_async_remote_copy(
            src_ref=src, dst_ref=hop.at[way, k, i],
            send_sem=h_send.at[way, k, i], recv_sem=h_recv.at[way, k, i],
            device_id=(to, col), device_id_type=MESH,
        )

    pair_lane = lax.broadcasted_iota(jnp.int32, (1, LANES), 1)
    first_half = pair_lane < samples

    def compute(i):
        slot = lax.rem(i, 3)
        fetch(i).wait()

        @pl.when(i + 2 < chunks)
        def _():
            fetch(i + 2).start()

        steps = group // STEP

        def one(j, carry):
            channel = i * group + j * STEP
            ratio = 1.0 + (0.5 / chan_whole) * (col * chan_local + channel).astype(jnp.float32)
            c, s = turn(delay[...] * ratio)
            base[0] = weight[...] * c
            base[1] = -weight[...] * s
            way = lax.div(j, steps // 2)
            inner = lax.rem(j, steps // 2)
            for p in range(STEP // 2):
                tiles = []
                for q in range(2):
                    real, imag = [], []
                    for k in range(fine.shape[3] // BLOCK):
                        cut = slice(k * BLOCK, (k + 1) * BLOCK)
                        keep = flags[k, channel + 2 * p + q].astype(jnp.float32)
                        br = fine[2 * p + q, 0, :, cut]
                        bi = fine[2 * p + q, 1, :, cut]
                        ar = base[0, :, cut] * keep
                        ai = base[1, :, cut] * keep
                        real.append((ar * br - ai * bi).astype(jnp.bfloat16))
                        imag.append((ar * bi + ai * br).astype(jnp.bfloat16))
                    tiles += [jnp.concatenate(real, axis=1), jnp.concatenate(imag, axis=1)]
                steer = jnp.concatenate(tiles, axis=0)
                at = pl.ds(pl.multiple_of(j * STEP * samples + p * LANES, LANES), LANES)
                signal = jnp.concatenate([vbuf[slot, 0, :, at], vbuf[slot, 1, :, at]], axis=1)
                out = jnp.dot(steer, signal, preferred_element_type=jnp.float32)
                beams = out.shape[0] // 4
                rr = [out[g * beams:(g + 1) * beams, :LANES] for g in range(4)]
                ri = [out[g * beams:(g + 1) * beams, LANES:] for g in range(4)]
                re = jnp.where(first_half, rr[0], rr[2]) - jnp.where(first_half, ri[1], ri[3])
                im = jnp.where(first_half, rr[1], rr[3]) + jnp.where(first_half, ri[0], ri[2])
                to = pl.ds(pl.multiple_of(inner * STEP * samples + p * LANES, LANES), LANES)
                for d in range(n):
                    own = slice(d * rows, (d + 1) * rows)
                    part[i, d % 2, way, d // 2, 0:rows, to] = re[own]
                    part[i, d % 2, way, d // 2, rows:2 * rows, to] = im[own]
            return carry

        lax.fori_loop(0, steps, one, 0)
        peer_copy(i).start()

    def pair_sum(i):
        peer_copy(i).wait_recv()
        for way in range(2):
            for d in range(chips):
                peer[i, way, d] = peer[i, way, d] + part[i, core, way, d]
        for way in range(2):
            hop_copy(i, way, 0).start()

    def forward(i, k):
        for way in range(2):
            hop_copy(i, way, k).wait_recv()
            block = lax.rem(chip + ((2 * chips - 2 - k) if way == 0 else (2 + k)), chips)
            hop[way, k, i] = hop[way, k, i] + peer[i, way, block]
            hop_copy(i, way, k + 1).start()

    def finish(i):
        per = LANES // group
        tile = counts_all[lax.div(i, per)]
        tile = pltpu.roll(tile, lax.rem(LANES - lax.rem(i, per) * group, LANES), 1)
        inverse = 1.0 / tile
        for way in range(2):
            k = chips - 2
            hop_copy(i, way, k).wait_recv()
            acc = jnp.zeros((rows, LANES), jnp.float32)
            for b in range(half // LANES):
                cut = slice(b * LANES, (b + 1) * LANES)
                v = hop[way, k, i, :, cut] + peer[i, way, chip, :, cut]
                c0 = way * (group // 2) + 2 * b
                scale = jnp.where(first_half, inverse[:rows, c0:c0 + 1], inverse[:rows, c0 + 1:c0 + 2])
                x = v[:rows] * scale
                y = v[rows:] * scale
                z = x * x + y * y
                power[:, pl.ds(pl.multiple_of(i * lanes + way * half + b * LANES, LANES), LANES)] = z
                acc = acc + z
            sums[pl.ds(col, 1)] = sums[pl.ds(col, 1)] + acc[None]

    last = 1 + gap * (chips - 1)

    def iteration(it, carry):
        done = it - last

        @pl.when(it == last)
        def _():
            acc = counts_part[me]
            for r in range(1, n):
                counts_copy(r).wait_recv()
                acc = acc + counts_in[r - 1]
            counts_all[...] = acc

        @pl.when(done >= 0)
        def _():
            finish(done)

        for k in range(chips - 3, -1, -1):
            at = it - 1 - gap * (k + 1)

            @pl.when((at >= 0) & (at < chunks))
            def _():
                forward(at, k)

        @pl.when((it >= 1) & (it - 1 < chunks))
        def _():
            pair_sum(it - 1)

        @pl.when(it < chunks)
        def _():
            compute(it)

        return carry

    lax.fori_loop(0, chunks + last, iteration, 0)

    def total_copy(r):
        return pltpu.make_async_remote_copy(
            src_ref=sums.at[col], dst_ref=sums.at[col],
            send_sem=t_send.at[r - 1], recv_sem=t_recv.at[r - 1],
            device_id=(me, lax.rem(col + r, nchan)), device_id_type=MESH,
        )

    def total_wait(r):
        src = lax.rem(col + nchan - r, nchan)
        pltpu.make_async_remote_copy(
            src_ref=sums.at[src], dst_ref=sums.at[src],
            send_sem=t_send.at[r - 1], recv_sem=t_recv.at[r - 1],
            device_id=(me, src), device_id_type=MESH,
        ).wait_recv()

    for r in range(1, nchan):
        total_copy(r).start()

    def drain(i, carry):
        peer_copy(i).wait_send()
        for way in range(2):
            for k in range(chips - 1):
                hop_copy(i, way, k).wait_send()
        return carry

    lax.fori_loop(0, chunks, drain, 0)
    for r in range(1, n):
        counts_copy(r).wait_send()
    for r in range(1, nchan):
        total_wait(r)
    acc = sums[0]
    for r in range(1, nchan):
        acc = acc + sums[r]
    total[...] = jnp.broadcast_to(jnp.sum(acc, axis=1, keepdims=True), (rows, LANES))
    for r in range(1, nchan):
        total_copy(r).wait_send()


def on_device(voltages, positions, directions, flag_mask, tapers, weight_index, group=32, gap=2):
    n, nchan = lax.axis_size("stn"), lax.axis_size("chan")
    blocks, chan_local = flag_mask.shape[1:]
    beams = directions.shape[1]
    dipoles = voltages.shape[2]
    samples = voltages.shape[3] // chan_local
    rows, chips = beams // n, n // 2
    chunks = chan_local // group
    half = group // 2 * samples
    place = positions[0]
    delay = (
        directions[0][:, None] * place[0][None, :]
        + directions[1][:, None] * place[1][None, :]
        + directions[2][:, None] * place[2][None, :]
    )
    choose = (weight_index[0][:, None] == jnp.arange(tapers.shape[1])[None, :]).astype(jnp.float32)
    weight = jnp.sum(choose * tapers[0][None, :], axis=1)
    alive = jnp.sum(flag_mask[0], axis=0).astype(jnp.float32) * BLOCK
    counts = (
        weight.reshape(n, 1, rows, 1) * alive.reshape(1, chan_local // LANES, 1, LANES)
    )
    crows = max(rows, 8)
    counts = jnp.concatenate(
        [counts, jnp.ones((n, chan_local // LANES, crows - rows, LANES), jnp.float32)], axis=2
    ) if crows > rows else counts
    dims = (n, nchan, chips, rows, chan_local, samples, group, chunks, half)
    f32 = jnp.float32
    vmem = pl.BlockSpec(memory_space=pltpu.VMEM)
    dma = pltpu.SemaphoreType.DMA
    power, total = pl.pallas_call(
        functools.partial(kernel, dims, gap),
        out_shape=(
            jax.ShapeDtypeStruct((rows, chan_local * samples), f32),
            jax.ShapeDtypeStruct((rows, LANES), f32),
        ),
        in_specs=[
            pl.BlockSpec(memory_space=pl.ANY),
            pl.BlockSpec(memory_space=pltpu.SMEM),
            vmem, vmem, vmem,
        ],
        out_specs=(vmem, vmem),
        scratch_shapes=[
            pltpu.VMEM((3, 2, dipoles, 2 * half), jnp.bfloat16),
            pltpu.VMEM((chunks, 2, 2, chips, 2 * rows, half), f32),
            pltpu.VMEM((chunks, 2, chips, 2 * rows, half), f32),
            pltpu.VMEM((2, chips - 1, chunks, 2 * rows, half), f32),
            pltpu.VMEM((2, beams, dipoles), f32),
            pltpu.VMEM((STEP, 2, beams, dipoles), f32),
            pltpu.VMEM((n - 1, chan_local // LANES, crows, LANES), f32),
            pltpu.VMEM((chan_local // LANES, crows, LANES), f32),
            pltpu.VMEM((nchan, rows, LANES), f32),
            dma((3,)),
            dma((chunks,)),
            dma((chunks,)),
            dma((2, chips - 1, chunks)),
            dma((2, chips - 1, chunks)),
            dma((n - 1,)),
            dma((n - 1,)),
            dma((nchan - 1,)),
            dma((nchan - 1,)),
        ],
        compiler_params=pltpu.CompilerParams(
            collective_id=0, has_side_effects=True, vmem_limit_bytes=60 * 1024 * 1024
        ),
    )(voltages[0], flag_mask[0], delay, jnp.broadcast_to(weight[:, None], delay.shape), counts)
    return power, total[:, 0]


def solution(mesh):
    in_specs = (
        P("stn", None, None, "chan"),
        P("stn", None, None),
        P(),
        P("stn", None, "chan"),
        P("stn", None),
        P("stn", None),
    )
    out_specs = (P("stn", "chan"), P("stn"))
    return jax.shard_map(
        on_device, mesh=mesh, in_specs=in_specs, out_specs=out_specs, check_vma=False
    )
```

```python
import functools
import math

import jax
import jax.numpy as jnp
from jax import lax
from jax.experimental import pallas as pl
from jax.experimental.pallas import tpu as pltpu
from jax.sharding import PartitionSpec as P

BLOCK = 128
LANES = 128
STEP = 8
MESH = pl.DeviceIdType.MESH


def turn(u):
    quarter = jnp.floor(u * 4.0 + 0.5)
    x = (u - quarter * 0.25) * (2.0 * math.pi)
    x2 = x * x
    s = x * (1.0 + x2 * (-1.0 / 6 + x2 * (1.0 / 120 + x2 * (-1.0 / 5040 + x2 * (1.0 / 362880)))))
    c = 1.0 + x2 * (-0.5 + x2 * (1.0 / 24 + x2 * (-1.0 / 720 + x2 * (1.0 / 40320))))
    q = quarter - 4.0 * jnp.floor(quarter * 0.25)
    odd = (q == 1.0) | (q == 3.0)
    cos = jnp.where(odd, s, c)
    sin = jnp.where(odd, c, s)
    cos = jnp.where((q == 1.0) | (q == 2.0), -cos, cos)
    sin = jnp.where(q >= 2.0, -sin, sin)
    return cos, sin


def kernel(
    dims, gap, volts, flags, delay, weight, counts_part, power, total,
    vbuf, part, peer, hop, base, fine, counts_in, counts_all, sums,
    v_sem, x_send, x_recv, h_send, h_recv, c_send, c_recv, t_send, t_recv,
):
    n, nchan, chips, rows, chan_local, samples, group, chunks, half = dims
    me = lax.axis_index("stn")
    col = lax.axis_index("chan")
    chip, core = lax.div(me, 2), lax.rem(me, 2)
    lanes = 2 * half

    def fetch(i):
        return pltpu.make_async_copy(
            volts.at[:, :, pl.ds(pl.multiple_of(i * lanes, lanes), lanes)],
            vbuf.at[lax.rem(i, 3)],
            v_sem.at[lax.rem(i, 3)],
        )

    for i in range(min(2, chunks)):
        fetch(i).start()

    barrier = pltpu.get_barrier_semaphore()
    for r in range(1, n):
        pl.semaphore_signal(barrier, 1, device_id=(lax.rem(me + r, n), col), device_id_type=MESH)
    for r in range(1, nchan):
        pl.semaphore_signal(barrier, 1, device_id=(me, lax.rem(col + r, nchan)), device_id_type=MESH)

    chan_whole = chan_local * nchan
    for i in range(STEP):
        c, s = turn(delay[...] * (0.5 * i / chan_whole))
        fine[i, 0] = c
        fine[i, 1] = -s
    sums[pl.ds(col, 1)] = jnp.zeros((1, rows, LANES), jnp.float32)

    pl.semaphore_wait(barrier, n - 1 + nchan - 1)

    def counts_copy(r):
        to = lax.rem(me + r, n)
        return pltpu.make_async_remote_copy(
            src_ref=counts_part.at[to], dst_ref=counts_in.at[r - 1],
            send_sem=c_send.at[r - 1], recv_sem=c_recv.at[r - 1],
            device_id=(to, col), device_id_type=MESH,
        )

    for r in range(1, n):
        counts_copy(r).start()

    def peer_copy(i):
        return pltpu.make_async_remote_copy(
            src_ref=part.at[i, 1 - core], dst_ref=peer.at[i],
            send_sem=x_send.at[i], recv_sem=x_recv.at[i],
            device_id=(chip * 2 + 1 - core, col), device_id_type=MESH,
        )

    def hop_copy(i, way, k):
        to = lax.rem(chip + (1 if way == 0 else chips - 1), chips) * 2 + core
        if k == 0:
            block = lax.rem(chip + (chips - 1 if way == 0 else 1), chips)
            src = peer.at[i, way, block]
        else:
            src = hop.at[way, k - 1, i]
        return pltpu.make_async_remote_copy(
            src_ref=src, dst_ref=hop.at[way, k, i],
            send_sem=h_send.at[way, k, i], recv_sem=h_recv.at[way, k, i],
            device_id=(to, col), device_id_type=MESH,
        )

    pair_lane = lax.broadcasted_iota(jnp.int32, (1, LANES), 1)
    first_half = pair_lane < samples

    def compute(i):
        slot = lax.rem(i, 3)
        fetch(i).wait()

        @pl.when(i + 2 < chunks)
        def _():
            fetch(i + 2).start()

        steps = group // STEP

        def one(j, carry):
            channel = i * group + j * STEP
            ratio = 1.0 + (0.5 / chan_whole) * (col * chan_local + channel).astype(jnp.float32)
            c, s = turn(delay[...] * ratio)
            base[0] = weight[...] * c
            base[1] = -weight[...] * s
            way = lax.div(j, steps // 2)
            inner = lax.rem(j, steps // 2)
            for p in range(STEP // 2):
                tiles = []
                for q in range(2):
                    real, imag = [], []
                    for k in range(fine.shape[3] // BLOCK):
                        cut = slice(k * BLOCK, (k + 1) * BLOCK)
                        keep = flags[k, channel + 2 * p + q].astype(jnp.float32)
                        br = fine[2 * p + q, 0, :, cut]
                        bi = fine[2 * p + q, 1, :, cut]
                        ar = base[0, :, cut] * keep
                        ai = base[1, :, cut] * keep
                        real.append((ar * br - ai * bi).astype(jnp.bfloat16))
                        imag.append((ar * bi + ai * br).astype(jnp.bfloat16))
                    tiles += [jnp.concatenate(real, axis=1), jnp.concatenate(imag, axis=1)]
                steer = jnp.concatenate(tiles, axis=0)
                at = pl.ds(pl.multiple_of(j * STEP * samples + p * LANES, LANES), LANES)
                signal = jnp.concatenate([vbuf[slot, 0, :, at], vbuf[slot, 1, :, at]], axis=1)
                out = jnp.dot(steer, signal, preferred_element_type=jnp.float32)
                beams = out.shape[0] // 4
                rr = [out[g * beams:(g + 1) * beams, :LANES] for g in range(4)]
                ri = [out[g * beams:(g + 1) * beams, LANES:] for g in range(4)]
                re = jnp.where(first_half, rr[0], rr[2]) - jnp.where(first_half, ri[1], ri[3])
                im = jnp.where(first_half, rr[1], rr[3]) + jnp.where(first_half, ri[0], ri[2])
                to = pl.ds(pl.multiple_of(inner * STEP * samples + p * LANES, LANES), LANES)
                for d in range(n):
                    own = slice(d * rows, (d + 1) * rows)
                    part[i, d % 2, way, d // 2, 0:rows, to] = re[own]
                    part[i, d % 2, way, d // 2, rows:2 * rows, to] = im[own]
            return carry

        lax.fori_loop(0, steps, one, 0)
        peer_copy(i).start()

    def pair_sum(i):
        peer_copy(i).wait_recv()
        for way in range(2):
            for d in range(chips):
                peer[i, way, d] = peer[i, way, d] + part[i, core, way, d]
        for way in range(2):
            hop_copy(i, way, 0).start()

    def forward(i, k):
        for way in range(2):
            hop_copy(i, way, k).wait_recv()
            block = lax.rem(chip + ((2 * chips - 2 - k) if way == 0 else (2 + k)), chips)
            hop[way, k, i] = hop[way, k, i] + peer[i, way, block]
            hop_copy(i, way, k + 1).start()

    def finish(i):
        per = LANES // group
        tile = counts_all[lax.div(i, per)]
        tile = pltpu.roll(tile, lax.rem(LANES - lax.rem(i, per) * group, LANES), 1)
        inverse = 1.0 / tile
        for way in range(2):
            k = chips - 2
            hop_copy(i, way, k).wait_recv()
            acc = jnp.zeros((rows, LANES), jnp.float32)
            for b in range(half // LANES):
                cut = slice(b * LANES, (b + 1) * LANES)
                v = hop[way, k, i, :, cut] + peer[i, way, chip, :, cut]
                c0 = way * (group // 2) + 2 * b
                scale = jnp.where(first_half, inverse[:rows, c0:c0 + 1], inverse[:rows, c0 + 1:c0 + 2])
                x = v[:rows] * scale
                y = v[rows:] * scale
                z = x * x + y * y
                power[:, pl.ds(pl.multiple_of(i * lanes + way * half + b * LANES, LANES), LANES)] = z
                acc = acc + z
            sums[pl.ds(col, 1)] = sums[pl.ds(col, 1)] + acc[None]

    last = 1 + gap * (chips - 1)

    def iteration(it, carry):
        done = it - last

        @pl.when(it == last)
        def _():
            acc = counts_part[me]
            for r in range(1, n):
                counts_copy(r).wait_recv()
                acc = acc + counts_in[r - 1]
            counts_all[...] = acc

        @pl.when(done >= 0)
        def _():
            finish(done)

        for k in range(chips - 3, -1, -1):
            at = it - 1 - gap * (k + 1)

            @pl.when((at >= 0) & (at < chunks))
            def _():
                forward(at, k)

        @pl.when((it >= 1) & (it - 1 < chunks))
        def _():
            pair_sum(it - 1)

        @pl.when(it < chunks)
        def _():
            compute(it)

        return carry

    lax.fori_loop(0, chunks + last, iteration, 0)

    def total_copy(r):
        return pltpu.make_async_remote_copy(
            src_ref=sums.at[col], dst_ref=sums.at[col],
            send_sem=t_send.at[r - 1], recv_sem=t_recv.at[r - 1],
            device_id=(me, lax.rem(col + r, nchan)), device_id_type=MESH,
        )

    def total_wait(r):
        src = lax.rem(col + nchan - r, nchan)
        pltpu.make_async_remote_copy(
            src_ref=sums.at[src], dst_ref=sums.at[src],
            send_sem=t_send.at[r - 1], recv_sem=t_recv.at[r - 1],
            device_id=(me, src), device_id_type=MESH,
        ).wait_recv()

    for r in range(1, nchan):
        total_copy(r).start()

    def drain(i, carry):
        peer_copy(i).wait_send()
        for way in range(2):
            for k in range(chips - 1):
                hop_copy(i, way, k).wait_send()
        return carry

    lax.fori_loop(0, chunks, drain, 0)
    for r in range(1, n):
        counts_copy(r).wait_send()
    for r in range(1, nchan):
        total_wait(r)
    acc = sums[0]
    for r in range(1, nchan):
        acc = acc + sums[r]
    total[...] = jnp.broadcast_to(jnp.sum(acc, axis=1, keepdims=True), (rows, LANES))
    for r in range(1, nchan):
        total_copy(r).wait_send()


def on_device(voltages, positions, directions, flag_mask, tapers, weight_index, group=16, gap=4):
    n, nchan = lax.axis_size("stn"), lax.axis_size("chan")
    blocks, chan_local = flag_mask.shape[1:]
    beams = directions.shape[1]
    dipoles = voltages.shape[2]
    samples = voltages.shape[3] // chan_local
    rows, chips = beams // n, n // 2
    chunks = chan_local // group
    half = group // 2 * samples
    place = positions[0]
    delay = (
        directions[0][:, None] * place[0][None, :]
        + directions[1][:, None] * place[1][None, :]
        + directions[2][:, None] * place[2][None, :]
    )
    choose = (weight_index[0][:, None] == jnp.arange(tapers.shape[1])[None, :]).astype(jnp.float32)
    weight = jnp.sum(choose * tapers[0][None, :], axis=1)
    alive = jnp.sum(flag_mask[0], axis=0).astype(jnp.float32) * BLOCK
    counts = (
        weight.reshape(n, 1, rows, 1) * alive.reshape(1, chan_local // LANES, 1, LANES)
    )
    crows = max(rows, 8)
    counts = jnp.concatenate(
        [counts, jnp.ones((n, chan_local // LANES, crows - rows, LANES), jnp.float32)], axis=2
    ) if crows > rows else counts
    dims = (n, nchan, chips, rows, chan_local, samples, group, chunks, half)
    f32 = jnp.float32
    vmem = pl.BlockSpec(memory_space=pltpu.VMEM)
    dma = pltpu.SemaphoreType.DMA
    power, total = pl.pallas_call(
        functools.partial(kernel, dims, gap),
        out_shape=(
            jax.ShapeDtypeStruct((rows, chan_local * samples), f32),
            jax.ShapeDtypeStruct((rows, LANES), f32),
        ),
        in_specs=[
            pl.BlockSpec(memory_space=pl.ANY),
            pl.BlockSpec(memory_space=pltpu.SMEM),
            vmem, vmem, vmem,
        ],
        out_specs=(vmem, vmem),
        scratch_shapes=[
            pltpu.VMEM((3, 2, dipoles, 2 * half), jnp.bfloat16),
            pltpu.VMEM((chunks, 2, 2, chips, 2 * rows, half), f32),
            pltpu.VMEM((chunks, 2, chips, 2 * rows, half), f32),
            pltpu.VMEM((2, chips - 1, chunks, 2 * rows, half), f32),
            pltpu.VMEM((2, beams, dipoles), f32),
            pltpu.VMEM((STEP, 2, beams, dipoles), f32),
            pltpu.VMEM((n - 1, chan_local // LANES, crows, LANES), f32),
            pltpu.VMEM((chan_local // LANES, crows, LANES), f32),
            pltpu.VMEM((nchan, rows, LANES), f32),
            dma((3,)),
            dma((chunks,)),
            dma((chunks,)),
            dma((2, chips - 1, chunks)),
            dma((2, chips - 1, chunks)),
            dma((n - 1,)),
            dma((n - 1,)),
            dma((nchan - 1,)),
            dma((nchan - 1,)),
        ],
        compiler_params=pltpu.CompilerParams(
            collective_id=0, has_side_effects=True, vmem_limit_bytes=60 * 1024 * 1024
        ),
    )(voltages[0], flag_mask[0], delay, jnp.broadcast_to(weight[:, None], delay.shape), counts)
    return power, total[:, 0]


def solution(mesh):
    in_specs = (
        P("stn", None, None, "chan"),
        P("stn", None, None),
        P(),
        P("stn", None, "chan"),
        P("stn", None),
        P("stn", None),
    )
    out_specs = (P("stn", "chan"), P("stn"))
    return jax.shard_map(
        on_device, mesh=mesh, in_specs=in_specs, out_specs=out_specs, check_vma=False
    )
```
